128 devices in a mesh: gx: 8 (over y, z_lo), gy: 16 (over z_hi, x, core).
Axes of the slice: x: 4, y: 4, z: 4 (z_hi: 2, z_lo: 2; z = z_hi * 2 + z_lo), core: 2. Of those that a mesh axis runs over, the one named last changes fastest.
Arguments:
- tokens: bfloat16 [8192, 8192], P('gy', 'gx'), may hold values from -6 to 6
- pair_ids: int32 [16], replicated, may hold values from 0 to 15, each once
- query_weight: bfloat16 [8192, 8192], P('gy', 'gx'), may hold values from -0.0625 to 0.0625
- key_matrix: bfloat16 [8192, 1024], P('gy', 'gx'), may hold values from -0.0625 to 0.0625
- value_matrix: bfloat16 [8192, 1024], P('gy', 'gx'), may hold values from -0.0625 to 0.0625
- query_bias: bfloat16 [8192], P('gx'), may hold values from -13 to 13
- key_bias: bfloat16 [1024], P('gx'), may hold values from -8 to 8
- value_offset_bias: bfloat16 [1024], P('gx'), may hold values from -3 to 3
Outputs:
- attn_out: bfloat16 [8192, 8192], P('gy', 'gx')
The draws below stay inside these ranges and needn't reach their ends.
Inputs may be any that keep to these rules, and one draw needn't show every extreme that they name: `pair_ids`: each number from 0 to 15 appears once.
All inputs are finite; a program needn't handle non-finite values.
Results may differ from the reference program's by a relative error of at most 0.0055.
The reference program's roundings to bfloat16 on the way count: a program that leaves them out, or rounds other values in their place, can miss the bound.
Values may be sent and summed in bfloat16 or wider, within the bound.
A program may use at most 128 MiB of HBM per device.

```python
import math
import jax
import jax.numpy as jnp
from jax import lax

MODEL_WIDTH = 8192
QUERY_HEADS = 64
KEY_VALUE_HEADS = 8
HEAD_SIZE = 128
TOK_DEV = 512
SEQ = 8192


def draw_query_bias(key, part):
    random_jitter = jnp.clip(0.5 * jax.random.normal(jax.random.fold_in(key, 11), (QUERY_HEADS, HEAD_SIZE), jnp.float32), -3.0, 3.0)
    return random_jitter.reshape(QUERY_HEADS * HEAD_SIZE).astype(jnp.bfloat16)


def draw_key_bias(key, part):
    random_jitter = jnp.clip(0.5 * jax.random.normal(jax.random.fold_in(key, 21), (KEY_VALUE_HEADS, HEAD_SIZE), jnp.float32), -3.0, 3.0)
    return random_jitter.reshape(KEY_VALUE_HEADS * HEAD_SIZE).astype(jnp.bfloat16)


def steps_of(rng, dims, pieces, smallest, top_value):
    def one(dim, parts):
        heights = jax.random.uniform(jax.random.fold_in(jax.random.fold_in(rng, 6), dim), (parts,), jnp.float32, smallest / len(pieces), top_value / len(pieces))
        return jnp.repeat(jnp.exp(heights), dims[dim] // parts).reshape((-1,) + (1,) * (len(dims) - dim - 1))

    level = one(*pieces[0])
    for cut in pieces[1:]:
        level = level * one(*cut)
    return level


def centred(rng, extent, scale, bound, cuts=(), kind=jnp.bfloat16):
    loudness = steps_of(rng, extent, cuts, -0.22, 0.18) if cuts else 1.0
    array = jax.random.normal(rng, extent, jnp.float32) * scale * loudness
    return jnp.minimum(jnp.maximum(array, -bound), bound).astype(kind)


def setup_inputs(seed: int = 0) -> dict:
    keys = jax.random.split(jax.random.key(seed), 9)
    tokens = centred(keys[0], (SEQ, MODEL_WIDTH), 1.0, 6.0, ((0, 16), (1, 8)))
    pair_ids = jax.random.permutation(keys[1], SEQ // TOK_DEV).astype(jnp.int32)
    query_weight = centred(keys[2], (MODEL_WIDTH, QUERY_HEADS * HEAD_SIZE), MODEL_WIDTH ** -0.5, 0.0625, ((0, 16), (1, 8)))
    key_matrix = centred(keys[3], (MODEL_WIDTH, KEY_VALUE_HEADS * HEAD_SIZE), MODEL_WIDTH ** -0.5, 0.0625, ((0, 16), (1, 8)))
    value_matrix = centred(keys[4], (MODEL_WIDTH, KEY_VALUE_HEADS * HEAD_SIZE), MODEL_WIDTH ** -0.5, 0.0625, ((0, 16), (1, 8)))
    query_bias = draw_query_bias(jax.random.fold_in(keys[8], 71), 0)
    key_bias = draw_key_bias(jax.random.fold_in(keys[8], 71), 0)
    value_offset_bias = centred(keys[7], (KEY_VALUE_HEADS * HEAD_SIZE,), 0.5, 3.0, ((0, 8),))
    return {"tokens": tokens, "pair_ids": pair_ids, "query_weight": query_weight, "key_matrix": key_matrix, "value_matrix": value_matrix, "query_bias": query_bias, "key_bias": key_bias, "value_offset_bias": value_offset_bias}


rope_theta = 1000000.0
neg_large = -1e+30

def table_lookup(entries, wanted):
    slot_ids = lax.iota(jnp.int32, entries.shape[0])
    return lax.optimization_barrier(jnp.sum(jnp.where(wanted[:, None] == slot_ids[None, :], entries[None, :], 0), axis=1)).astype(jnp.int32)

def layout_positions(pair_ids, total_row_count, tok_dev):
    half_len = tok_dev // 2
    row_ids = lax.iota(jnp.int32, total_row_count)
    within = row_ids % tok_dev
    owners = table_lookup(pair_ids, row_ids // tok_dev)
    mirrored = 2 * pair_ids.shape[0] - 1 - owners
    return jnp.where(within < half_len, owners * half_len + within, mirrored * half_len + within - half_len).astype(jnp.int32)

def apply_rotary(values, token_positions):
    half_size = values.shape[-1] // 2
    frequency = jnp.exp(lax.iota(jnp.float32, half_size) * (-2.0 * math.log(rope_theta) / values.shape[-1]))
    angles = token_positions.astype(jnp.float32)[:, None] * frequency[None, :]
    cos_part = jnp.cos(angles)[:, None, :]
    sin_part = jnp.sin(angles)[:, None, :]
    lower_half = values[..., :half_size]
    upper_half = values[..., half_size:]
    return jnp.concatenate([lower_half * cos_part - upper_half * sin_part, upper_half * cos_part + lower_half * sin_part], axis=-1)

def reference(tokens, pair_ids, query_weight, key_matrix, value_matrix, query_bias, key_bias, value_offset_bias):
    total_row_count = tokens.shape[0]
    token_positions = layout_positions(pair_ids, total_row_count, TOK_DEV)
    queries = jnp.dot(tokens, query_weight, preferred_element_type=jnp.float32) + query_bias.astype(jnp.float32)
    queries = apply_rotary(queries.reshape(total_row_count, QUERY_HEADS, HEAD_SIZE), token_positions).astype(jnp.bfloat16)
    projected_key_rows = jnp.dot(tokens, key_matrix, preferred_element_type=jnp.float32) + key_bias.astype(jnp.float32)
    projected_key_rows = apply_rotary(projected_key_rows.reshape(total_row_count, KEY_VALUE_HEADS, HEAD_SIZE), token_positions).astype(jnp.bfloat16)
    projected_value_rows = (jnp.dot(tokens, value_matrix, preferred_element_type=jnp.float32) + value_offset_bias.astype(jnp.float32)).astype(jnp.bfloat16)
    projected_value_rows = projected_value_rows.reshape(total_row_count, KEY_VALUE_HEADS, HEAD_SIZE)
    visible = token_positions[None, :] <= token_positions[:, None]
    query_group_width = QUERY_HEADS // KEY_VALUE_HEADS
    scale = 1.0 / math.sqrt(HEAD_SIZE)

    def one_head(head_id):
        query_head = lax.dynamic_index_in_dim(queries, head_id, 1, keepdims=False)
        kv_head = head_id // query_group_width
        key_head = lax.dynamic_index_in_dim(projected_key_rows, kv_head, 1, keepdims=False)
        value_head = lax.dynamic_index_in_dim(projected_value_rows, kv_head, 1, keepdims=False)
        scores = jnp.dot(query_head, key_head.T, preferred_element_type=jnp.float32) * scale
        scores = jnp.where(visible, scores, neg_large)
        row_peak = lax.optimization_barrier(jnp.max(scores, axis=-1))
        probs = jnp.where(visible, jnp.exp(scores - row_peak[:, None]), 0.0)
        totals = lax.optimization_barrier(jnp.sum(probs, axis=-1))
        mixed = jnp.dot(probs.astype(jnp.bfloat16), value_head, preferred_element_type=jnp.float32)
        return (mixed / totals[:, None]).astype(jnp.bfloat16)
    outputs = lax.map(one_head, jnp.arange(QUERY_HEADS, dtype=jnp.int32))
    return outputs.transpose(1, 0, 2).reshape(total_row_count, QUERY_HEADS * HEAD_SIZE)
```

```python
import functools
import math

import jax
import jax.numpy as jnp
from jax import lax
from jax.experimental import pallas as pl
from jax.experimental.pallas import tpu as pltpu
from jax.sharding import PartitionSpec as P

THETA = 1000000.0
EXP2_SCALE = math.log2(math.e) / math.sqrt(128)
NEG = -1e30
MESH = pl.DeviceIdType.MESH

XS = 4
SLOTS = 7
S_E, S_L = 5, 6
KT = 1024
VIA_Z = (4, 16)


def kernel(
    pair_ref, x_hbm, wq_hbm, wk_hbm, wv_hbm, bq_ref, bk_ref, bv_ref,
    q_out, kv_out, m_out, l_out, o_out,
    xb, wb, kvb, qs, acc, cos_t, sin_t, st_m, st_l, st_o, loc_sem, out_sem, ws, wr, xs, xr,
):
    gx, gy = lax.axis_index("gx"), lax.axis_index("gy")
    y, zl = gx // 2, gx % 2
    zh, x, c = gy // 8, (gy // 2) % 4, gy % 2

    def at(dx=0, dy=0, dzh=0, dzl=0, dc=0):
        return (
            ((y + dy) % 4) * 2 + (zl + dzl) % 2,
            (((zh + dzh) % 2) * 4 + (x + dx) % 4) * 2 + (c + dc) % 2,
        )

    core, xp, xm, yp, ym, zfar, znear = (
        at(dc=1), at(dx=1), at(dx=3), at(dy=1), at(dy=3), at(dzh=1), at(dzl=1)
    )

    def block(plane, dx, dc=0):
        return (((zh + plane) % 2) * 4 + (x + dx) % 4) * 2 + (c + dc) % 2

    def xblock(plane, dy):
        return ((y + dy) % 4) * 2 + (zl + plane) % 2

    local = []

    def load(src, dst, n):
        cp = pltpu.make_async_copy(src, dst, loc_sem.at[n])
        cp.start()
        local.append(cp)

    load(wk_hbm, wb.at[0, gy, :, pl.ds(0, 128)], 0)
    load(wv_hbm, wb.at[0, gy, :, pl.ds(128, 128)], 1)
    for r in range(XS):
        load(x_hbm.at[pl.ds(r * 128, 128)], xb.at[r, gx], 2 + r)
    for t in range(1, 5):
        load(wq_hbm.at[:, pl.ds((t - 1) * 256, 256)], wb.at[t, gy], 5 + t)

    barrier = pltpu.get_barrier_semaphore()
    for n in (core, xp, xm, yp, ym, zfar, znear):
        pl.semaphore_signal(barrier, inc=1, device_id=n, device_id_type=MESH)
    pl.semaphore_wait(barrier, 7)

    sends = []

    def send(src, dst, ssem, rsem, dev):
        cp = pltpu.make_async_remote_copy(
            src_ref=src, dst_ref=dst, send_sem=ssem, recv_sem=rsem, device_id=dev,
            device_id_type=MESH,
        )
        cp.start()
        sends.append(cp)

    def arrived(ref, sem):
        pltpu.make_async_copy(ref, ref, sem).wait()

    def blk(s, j):
        return wb.at[s, j] if s < S_E else kvb.at[s - S_E, j]

    def cuts(s):
        n = 512 if s < S_E else 256
        v = n * VIA_Z[0] // VIA_Z[1]
        return pl.ds(0, n // 2), pl.ds(n // 2, n // 2), pl.ds(0, n - v), pl.ds(n - v, v)

    P0, OM, OP, PM, PP, PMV, PPV, O2A, O2B, P2A, P2B, D = range(12)
    doff = {(0, 0): 0, (0, 3): 1, (0, 1): 2, (1, 0): 3, (1, 3): 4, (1, 1): 5, (0, 2): 6, (1, 2): 7}

    def wsend(s, ref, role, dev):
        send(ref, ref, ws.at[s, role], wr.at[s, role], dev)

    def d2d(s, plane, dx):
        wsend(s, blk(s, block(plane, dx)), D + doff[(plane, dx)], core)

    def own(s):
        b = blk(s, gy)
        wsend(s, b, P0, zfar)
        wsend(s, b, OM, xp)
        wsend(s, b, OP, xm)
        d2d(s, 0, 0)

    def relay_own(s):
        lo, hi, u, v = cuts(s)
        b = blk(s, block(0, 3))
        arrived(b, wr.at[s, OM])
        wsend(s, b.at[lo], O2A, xp)
        wsend(s, b.at[v], PMV, zfar)
        d2d(s, 0, 3)
        b = blk(s, block(0, 1))
        arrived(b, wr.at[s, OP])
        wsend(s, b.at[hi], O2B, xm)
        wsend(s, b.at[v], PPV, zfar)
        d2d(s, 0, 1)

    def partner(s):
        lo, hi, u, v = cuts(s)
        b = blk(s, block(1, 0))
        arrived(b, wr.at[s, P0])
        wsend(s, b.at[u], PM, xp)
        wsend(s, b.at[u], PP, xm)
        d2d(s, 1, 0)

    def relay_partner(s):
        lo, hi, u, v = cuts(s)
        b = blk(s, block(1, 3))
        arrived(b.at[u], wr.at[s, PM])
        arrived(b.at[v], wr.at[s, PMV])
        wsend(s, b.at[lo], P2A, xp)
        d2d(s, 1, 3)
        b = blk(s, block(1, 1))
        arrived(b.at[u], wr.at[s, PP])
        arrived(b.at[v], wr.at[s, PPV])
        wsend(s, b.at[hi], P2B, xm)
        d2d(s, 1, 1)

    def last(s):
        lo, hi, u, v = cuts(s)
        for plane, ra, rb in ((0, O2A, O2B), (1, P2A, P2B)):
            b = blk(s, block(plane, 2))
            arrived(b.at[lo], wr.at[s, ra])
            arrived(b.at[hi], wr.at[s, rb])
            d2d(s, plane, 2)

    def other_core(s):
        for (plane, dx), d in doff.items():
            arrived(blk(s, block(plane, dx, 1)), wr.at[s, D + d])

    XZ, XOM, XOP, XPM, XPP, XO2A, XO2B, XP2A, XP2B = range(9)
    xlo, xhi = pl.ds(0, 64), pl.ds(64, 64)

    def xsend(t, ref, role, dev):
        send(ref, ref, xs.at[t, role], xr.at[t, role], dev)

    def xown(t):
        b = xb.at[t, gx]
        xsend(t, b, XZ, znear)
        xsend(t, b, XOM, yp)
        xsend(t, b, XOP, ym)

    def xrelay(t, plane):
        rm, rp, ra, rb = (XOM, XOP, XO2A, XO2B) if plane == 0 else (XPM, XPP, XP2A, XP2B)
        b = xb.at[t, xblock(plane, 3)]
        arrived(b, xr.at[t, rm])
        xsend(t, b.at[xlo], ra, yp)
        b = xb.at[t, xblock(plane, 1)]
        arrived(b, xr.at[t, rp])
        xsend(t, b.at[xhi], rb, ym)

    def xpartner(t):
        b = xb.at[t, xblock(1, 0)]
        arrived(b, xr.at[t, XZ])
        xsend(t, b, XPM, yp)
        xsend(t, b, XPP, ym)

    def xlast(t):
        for plane, ra, rb in ((0, XO2A, XO2B), (1, XP2A, XP2B)):
            b = xb.at[t, xblock(plane, 2)]
            arrived(b.at[xlo], xr.at[t, ra])
            arrived(b.at[xhi], xr.at[t, rb])

    def project(s, half):
        total = None
        for b in range(8):
            part = jnp.dot(
                xb[pl.ds(2 * half, 2), b].reshape(256, 1024),
                wb[s, pl.ds(2 * b, 2)].reshape(1024, 256),
                preferred_element_type=jnp.float32,
            )
            total = part if total is None else total + part
        acc[...] = total

    def rope(u, half):
        r = pl.ds(half * 256, 256)
        return u * cos_t[r, :] + pltpu.roll(u, 64, 1) * sin_t[r, :]

    def make_kv(half):
        project(0, half)
        kvb[half, gy, :, 0:128] = rope(
            acc[:, 0:128] + bk_ref[...].astype(jnp.float32), half
        ).astype(jnp.bfloat16)
        kvb[half, gy, :, 128:256] = (
            acc[:, 128:256] + bv_ref[...].astype(jnp.float32)
        ).astype(jnp.bfloat16)

    def make_q(hp, half):
        project(hp + 1, half)
        for g in range(2):
            h = 2 * hp + g
            u = acc[:, g * 128:(g + 1) * 128] + bq_ref[:, h * 128:(h + 1) * 128].astype(jnp.float32)
            qs[half, pl.ds(h * 256, 256), :] = rope(u, half).astype(jnp.bfloat16)

    def tables():
        p = pair_ref[gy]
        row = lax.broadcasted_iota(jnp.int32, (512, 128), 0)
        pos = jnp.where(row < 256, p * 256 + row, (31 - p) * 256 + row - 256)
        lane = lax.broadcasted_iota(jnp.int32, (512, 128), 1)
        half = (lane % 64).astype(jnp.float32)
        freq = jnp.exp(half * (-2.0 * math.log(THETA) / 128))
        ang = pos.astype(jnp.float32) * freq
        cos_t[...] = jnp.cos(ang)
        s = jnp.sin(ang)
        sin_t[...] = jnp.where(lane < 64, -s, s)

    outs = []

    def put(src, dst, n):
        cp = pltpu.make_async_copy(src, dst, out_sem.at[n])
        cp.start()
        outs.append(cp)

    def put_kv(half):
        put(kvb.at[half], kv_out.at[half], half)

    def put_state(hp):
        put(st_m.at[hp], m_out.at[hp], 3 + hp)
        put(st_l.at[hp], l_out.at[hp], 7 + hp)
        put(st_o.at[hp], o_out.at[hp], 11 + hp)

    def attend(hp):
        q = qs[1, pl.ds(hp * 512, 512), :]
        carry = (
            jnp.full((512, 1), NEG, jnp.float32),
            jnp.zeros((512, 128), jnp.float32),
            jnp.zeros((512, 128), jnp.float32),
        )
        m, l, o = lax.fori_loop(0, 4, lambda t, st: absorb(q, kvb, 0, t, st, None), carry)
        st_m[hp] = jnp.broadcast_to(m, (512, 128))
        st_l[hp] = l
        st_o[hp] = o

    local[0].wait()
    local[1].wait()
    own(0)
    local[2].wait()
    xown(0)
    for cp in local[3:]:
        cp.wait()
    tables()
    own(1)
    xown(1)
    relay_own(0)
    xrelay(0, 0)
    xpartner(0)
    partner(0)
    own(2)
    xown(2)
    xrelay(0, 1)
    xrelay(1, 0)
    xpartner(1)
    relay_partner(0)
    relay_own(1)
    partner(1)
    last(0)
    xlast(0)
    own(3)
    xown(3)
    xrelay(1, 1)
    xrelay(2, 0)
    xpartner(2)
    relay_partner(1)
    relay_own(2)
    partner(2)
    other_core(0)
    xlast(1)
    make_kv(0)
    last(1)
    own(S_E)
    xrelay(2, 1)
    xrelay(3, 0)
    xpartner(3)
    relay_partner(2)
    relay_own(3)
    relay_own(S_E)
    partner(S_E)
    partner(3)
    own(4)
    other_core(1)
    make_q(0, 0)
    xrelay(3, 1)
    last(2)
    xlast(2)
    relay_partner(S_E)
    relay_partner(3)
    other_core(2)
    make_q(1, 0)
    relay_own(4)
    partner(4)
    last(S_E)
    other_core(S_E)
    put_kv(0)
    xlast(3)
    make_kv(1)
    last(3)
    make_q(0, 1)
    own(S_L)
    relay_partner(4)
    make_q(1, 1)
    other_core(3)
    make_q(2, 0)
    relay_own(S_L)
    partner(S_L)
    make_q(2, 1)
    attend(0)
    relay_partner(S_L)
    last(4)
    attend(1)
    last(S_L)
    put_state(0)
    attend(2)
    other_core(4)
    make_q(3, 0)
    make_q(3, 1)
    other_core(S_L)
    put_kv(1)
    put_state(1)
    attend(3)
    put_state(2)
    put_state(3)
    put(qs, q_out, 2)
    for cp in sends:
        cp.wait_send()
    for cp in outs:
        cp.wait()


def absorb(q, kv, seg, t, state, vis):
    m, l, o = state
    kt = kv[seg, pl.ds(t * 4, 4), :, 0:128].reshape(KT, 128)
    vt = kv[seg, pl.ds(t * 4, 4), :, 128:256].reshape(KT, 128)
    s = lax.dot_general(q, kt, (((1,), (1,)), ((), ())), preferred_element_type=jnp.float32)
    if vis is not None:
        s = jnp.where(vis, s, NEG)
    mx = s[:, 0:128]
    for u in range(1, KT // 128):
        mx = jnp.maximum(mx, s[:, u * 128:(u + 1) * 128])
    mnew = jnp.maximum(m, jnp.max(mx, axis=1, keepdims=True) * EXP2_SCALE)
    pr = jnp.exp2(s * EXP2_SCALE - mnew)
    a = jnp.exp2(m - mnew)
    ps = pr[:, 0:128]
    for u in range(1, KT // 128):
        ps = ps + pr[:, u * 128:(u + 1) * 128]
    l = l * a + ps
    o = o * a + jnp.dot(pr.astype(jnp.bfloat16), vt, preferred_element_type=jnp.float32)
    return mnew, l, o


def gather_project(pair_ids, tokens, wq, wk, wv, bq, bk, bv):
    vmem = pl.BlockSpec(memory_space=pltpu.VMEM)
    hbm = pl.BlockSpec(memory_space=pl.ANY)
    state = jax.ShapeDtypeStruct((4, 512, 128), jnp.float32)
    return pl.pallas_call(
        kernel,
        out_shape=(
            jax.ShapeDtypeStruct((2, 2048, 128), jnp.bfloat16),
            jax.ShapeDtypeStruct((2, 16, 256, 256), jnp.bfloat16),
            state, state, state,
        ),
        in_specs=[pl.BlockSpec(memory_space=pltpu.SMEM), hbm, hbm, hbm, hbm, vmem, vmem, vmem],
        out_specs=(hbm,) * 5,
        scratch_shapes=[
            pltpu.VMEM((XS, 8, 128, 1024), jnp.bfloat16),
            pltpu.VMEM((5, 16, 512, 256), jnp.bfloat16),
            pltpu.VMEM((2, 16, 256, 256), jnp.bfloat16),
            pltpu.VMEM((2, 2048, 128), jnp.bfloat16),
            pltpu.VMEM((256, 256), jnp.float32),
            pltpu.VMEM((512, 128), jnp.float32),
            pltpu.VMEM((512, 128), jnp.float32),
            pltpu.VMEM((4, 512, 128), jnp.float32),
            pltpu.VMEM((4, 512, 128), jnp.float32),
            pltpu.VMEM((4, 512, 128), jnp.float32),
            pltpu.SemaphoreType.DMA((10,)),
            pltpu.SemaphoreType.DMA((15,)),
            pltpu.SemaphoreType.DMA((SLOTS, 19)),
            pltpu.SemaphoreType.DMA((SLOTS, 19)),
            pltpu.SemaphoreType.DMA((XS, 9)),
            pltpu.SemaphoreType.DMA((XS, 9)),
        ],
        compiler_params=pltpu.CompilerParams(
            collective_id=0, has_side_effects=True, vmem_limit_bytes=63 * 2**20
        ),
    )(pair_ids, tokens, wq, wk, wv, bq.reshape(1, -1), bk.reshape(1, -1), bv.reshape(1, -1))


def attn_kernel(pair_ref, q_hbm, kv_hbm, m_hbm, l_hbm, o_hbm, out_ref, q, kv, m0, l0, o0, sem, *, G):
    def cp(half, j):
        slot = pair_ref[j] if half == 0 else 15 - pair_ref[j]
        return pltpu.make_async_copy(kv_hbm.at[half, j], kv.at[half, slot], sem.at[half, j])

    rest = [
        pltpu.make_async_copy(a, b, sem.at[2, n])
        for n, (a, b) in enumerate(
            ((q_hbm.at[0], q.at[0]), (q_hbm.at[1], q.at[1]), (m_hbm, m0), (l_hbm, l0), (o_hbm, o0))
        )
    ]
    rest[0].start()
    for half in range(2):

        @pl.loop(0, 16)
        def _(j):
            cp(half, j).start()

        for r in rest[1:] if half else ():
            r.start()
    p = pair_ref[lax.axis_index("gy")]
    R = G * 256
    for half in range(2):

        @pl.loop(0, 16)
        def _(j):
            cp(half, j).wait()

        for r in rest[1:] if half else rest[:1]:
            r.wait()
        blk = p if half == 0 else 15 - p
        full = blk // 4

        @pl.loop(0, 8 // G)
        def _(i):
            rows = pl.ds(pl.multiple_of(i * R, R), R)
            qt = q[half, rows, :]
            if half:
                parts = [
                    jnp.concatenate([r[i * (G // 2) + g] for g in range(G // 2)], axis=0)
                    for r in (m0, l0, o0)
                ]
                state = (parts[0][:, 0:1], parts[1], parts[2])
            else:
                state = (
                    jnp.full((R, 1), NEG, jnp.float32),
                    jnp.zeros((R, 128), jnp.float32),
                    jnp.zeros((R, 128), jnp.float32),
                )
            ahead = lax.broadcasted_iota(jnp.int32, (R, KT), 1) - (
                lax.broadcasted_iota(jnp.int32, (R, KT), 0) % 256
            )
            state = absorb(qt, kv, half, full, state, ahead <= (blk - full * 4) * 256)
            m, l, o = lax.fori_loop(
                0, full, lambda t, st: absorb(qt, kv, half, t, st, None), state
            )
            o = (o / jnp.sum(l, axis=1, keepdims=True)).astype(jnp.bfloat16)
            for g in range(G):
                out_ref[half * 256:(half + 1) * 256, pl.ds(pl.multiple_of((i * G + g) * 128, 128), 128)] = (
                    o[g * 256:(g + 1) * 256]
                )


def on_device(tokens, pair_ids, wq, wk, wv, bq, bk, bv):
    q, kv, m, l, o = gather_project(pair_ids, tokens, wq, wk, wv, bq, bk, bv)
    hbm = pl.BlockSpec(memory_space=pl.ANY)
    return pl.pallas_call(
        functools.partial(attn_kernel, G=4),
        out_shape=jax.ShapeDtypeStruct((512, 1024), jnp.bfloat16),
        in_specs=[pl.BlockSpec(memory_space=pltpu.SMEM)] + [hbm] * 5,
        out_specs=pl.BlockSpec(memory_space=pltpu.VMEM),
        scratch_shapes=[
            pltpu.VMEM((2, 2048, 128), jnp.bfloat16),
            pltpu.VMEM((2, 16, 256, 256), jnp.bfloat16),
            pltpu.VMEM((4, 512, 128), jnp.float32),
            pltpu.VMEM((4, 512, 128), jnp.float32),
            pltpu.VMEM((4, 512, 128), jnp.float32),
            pltpu.SemaphoreType.DMA((3, 16)),
        ],
        compiler_params=pltpu.CompilerParams(vmem_limit_bytes=60 * 2**20),
    )(pair_ids, q, kv, m, l, o)


def solution(mesh):
    placed = (P("gy", "gx"), P(), P("gy", "gx"), P("gy", "gx"), P("gy", "gx"), P("gx"), P("gx"), P("gx"))
    return jax.shard_map(
        on_device, mesh=mesh, in_specs=placed, out_specs=P("gy", "gx"), check_vma=False
    )
```

```python
import functools
import math

import jax
import jax.numpy as jnp
from jax import lax
from jax.experimental import pallas as pl
from jax.experimental.pallas import tpu as pltpu
from jax.sharding import PartitionSpec as P

THETA = 1000000.0
EXP2_SCALE = math.log2(math.e) / math.sqrt(128)
NEG = -1e30
MESH = pl.DeviceIdType.MESH

XS = 4
SLOTS = 7
S_E, S_L = 5, 6
KT = 1024
VIA_Z = (4, 16)


def kernel(
    pair_ref, x_hbm, wq_hbm, wk_hbm, wv_hbm, bq_ref, bk_ref, bv_ref,
    q_out, kv_out, m_out, l_out, o_out,
    xb, wb, kvb, qs, acc, cos_t, sin_t, st_m, st_l, st_o, loc_sem, out_sem, ws, wr, xs, xr,
):
    gx, gy = lax.axis_index("gx"), lax.axis_index("gy")
    y, zl = gx // 2, gx % 2
    zh, x, c = gy // 8, (gy // 2) % 4, gy % 2

    def at(dx=0, dy=0, dzh=0, dzl=0, dc=0):
        return (
            ((y + dy) % 4) * 2 + (zl + dzl) % 2,
            (((zh + dzh) % 2) * 4 + (x + dx) % 4) * 2 + (c + dc) % 2,
        )

    core, xp, xm, yp, ym, zfar, znear = (
        at(dc=1), at(dx=1), at(dx=3), at(dy=1), at(dy=3), at(dzh=1), at(dzl=1)
    )

    def block(plane, dx, dc=0):
        return (((zh + plane) % 2) * 4 + (x + dx) % 4) * 2 + (c + dc) % 2

    def xblock(plane, dy):
        return ((y + dy) % 4) * 2 + (zl + plane) % 2

    local = []

    def load(src, dst, n):
        cp = pltpu.make_async_copy(src, dst, loc_sem.at[n])
        cp.start()
        local.append(cp)

    load(wk_hbm, wb.at[0, gy, :, pl.ds(0, 128)], 0)
    load(wv_hbm, wb.at[0, gy, :, pl.ds(128, 128)], 1)
    for r in range(XS):
        load(x_hbm.at[pl.ds(r * 128, 128)], xb.at[r, gx], 2 + r)
    for t in range(1, 5):
        load(wq_hbm.at[:, pl.ds((t - 1) * 256, 256)], wb.at[t, gy], 5 + t)

    barrier = pltpu.get_barrier_semaphore()
    for n in (core, xp, xm, yp, ym, zfar, znear):
        pl.semaphore_signal(barrier, inc=1, device_id=n, device_id_type=MESH)
    pl.semaphore_wait(barrier, 7)

    sends = []

    def send(src, dst, ssem, rsem, dev):
        cp = pltpu.make_async_remote_copy(
            src_ref=src, dst_ref=dst, send_sem=ssem, recv_sem=rsem, device_id=dev,
            device_id_type=MESH,
        )
        cp.start()
        sends.append(cp)

    def arrived(ref, sem):
        pltpu.make_async_copy(ref, ref, sem).wait()

    def blk(s, j):
        return wb.at[s, j] if s < S_E else kvb.at[s - S_E, j]

    def cuts(s):
        n = 512 if s < S_E else 256
        v = n * VIA_Z[0] // VIA_Z[1]
        return pl.ds(0, n // 2), pl.ds(n // 2, n // 2), pl.ds(0, n - v), pl.ds(n - v, v)

    P0, OM, OP, PM, PP, PMV, PPV, O2A, O2B, P2A, P2B, D = range(12)
    doff = {(0, 0): 0, (0, 3): 1, (0, 1): 2, (1, 0): 3, (1, 3): 4, (1, 1): 5, (0, 2): 6, (1, 2): 7}

    def wsend(s, ref, role, dev):
        send(ref, ref, ws.at[s, role], wr.at[s, role], dev)

    def d2d(s, plane, dx):
        wsend(s, blk(s, block(plane, dx)), D + doff[(plane, dx)], core)

    def own(s):
        b = blk(s, gy)
        wsend(s, b, P0, zfar)
        wsend(s, b, OM, xp)
        wsend(s, b, OP, xm)
        d2d(s, 0, 0)

    def relay_own(s):
        lo, hi, u, v = cuts(s)
        b = blk(s, block(0, 3))
        arrived(b, wr.at[s, OM])
        wsend(s, b.at[lo], O2A, xp)
        wsend(s, b.at[v], PMV, zfar)
        d2d(s, 0, 3)
        b = blk(s, block(0, 1))
        arrived(b, wr.at[s, OP])
        wsend(s, b.at[hi], O2B, xm)
        wsend(s, b.at[v], PPV, zfar)
        d2d(s, 0, 1)

    def partner(s):
        lo, hi, u, v = cuts(s)
        b = blk(s, block(1, 0))
        arrived(b, wr.at[s, P0])
        wsend(s, b.at[u], PM, xp)
        wsend(s, b.at[u], PP, xm)
        d2d(s, 1, 0)

    def relay_partner(s):
        lo, hi, u, v = cuts(s)
        b = blk(s, block(1, 3))
        arrived(b.at[u], wr.at[s, PM])
        arrived(b.at[v], wr.at[s, PMV])
        wsend(s, b.at[lo], P2A, xp)
        d2d(s, 1, 3)
        b = blk(s, block(1, 1))
        arrived(b.at[u], wr.at[s, PP])
        arrived(b.at[v], wr.at[s, PPV])
        wsend(s, b.at[hi], P2B, xm)
        d2d(s, 1, 1)

    def last(s):
        lo, hi, u, v = cuts(s)
        for plane, ra, rb in ((0, O2A, O2B), (1, P2A, P2B)):
            b = blk(s, block(plane, 2))
            arrived(b.at[lo], wr.at[s, ra])
            arrived(b.at[hi], wr.at[s, rb])
            d2d(s, plane, 2)

    def other_core(s):
        for (plane, dx), d in doff.items():
            arrived(blk(s, block(plane, dx, 1)), wr.at[s, D + d])

    XZ, XOM, XOP, XPM, XPP, XO2A, XO2B, XP2A, XP2B = range(9)
    xlo, xhi = pl.ds(0, 64), pl.ds(64, 64)

    def xsend(t, ref, role, dev):
        send(ref, ref, xs.at[t, role], xr.at[t, role], dev)

    def xown(t):
        b = xb.at[t, gx]
        xsend(t, b, XZ, znear)
        xsend(t, b, XOM, yp)
        xsend(t, b, XOP, ym)

    def xrelay(t, plane):
        rm, rp, ra, rb = (XOM, XOP, XO2A, XO2B) if plane == 0 else (XPM, XPP, XP2A, XP2B)
        b = xb.at[t, xblock(plane, 3)]
        arrived(b, xr.at[t, rm])
        xsend(t, b.at[xlo], ra, yp)
        b = xb.at[t, xblock(plane, 1)]
        arrived(b, xr.at[t, rp])
        xsend(t, b.at[xhi], rb, ym)

    def xpartner(t):
        b = xb.at[t, xblock(1, 0)]
        arrived(b, xr.at[t, XZ])
        xsend(t, b, XPM, yp)
        xsend(t, b, XPP, ym)

    def xlast(t):
        for plane, ra, rb in ((0, XO2A, XO2B), (1, XP2A, XP2B)):
            b = xb.at[t, xblock(plane, 2)]
            arrived(b.at[xlo], xr.at[t, ra])
            arrived(b.at[xhi], xr.at[t, rb])

    def project(s, half):
        total = None
        for b in range(8):
            part = jnp.dot(
                xb[pl.ds(2 * half, 2), b].reshape(256, 1024),
                wb[s, pl.ds(2 * b, 2)].reshape(1024, 256),
                preferred_element_type=jnp.float32,
            )
            total = part if total is None else total + part
        acc[...] = total

    def rope(u, half):
        r = pl.ds(half * 256, 256)
        return u * cos_t[r, :] + pltpu.roll(u, 64, 1) * sin_t[r, :]

    def make_kv(half):
        project(0, half)
        kvb[half, gy, :, 0:128] = rope(
            acc[:, 0:128] + bk_ref[...].astype(jnp.float32).reshape(1, 128), half
        ).astype(jnp.bfloat16)
        kvb[half, gy, :, 128:256] = (
            acc[:, 128:256] + bv_ref[...].astype(jnp.float32).reshape(1, 128)
        ).astype(jnp.bfloat16)

    def make_q(hp, half):
        project(hp + 1, half)
        for g in range(2):
            h = 2 * hp + g
            u = acc[:, g * 128:(g + 1) * 128] + bq_ref[h * 128:(h + 1) * 128].astype(jnp.float32).reshape(1, 128)
            qs[half, pl.ds(h * 256, 256), :] = rope(u, half).astype(jnp.bfloat16)

    def tables():
        p = pair_ref[gy]
        row = lax.broadcasted_iota(jnp.int32, (512, 128), 0)
        pos = jnp.where(row < 256, p * 256 + row, (31 - p) * 256 + row - 256)
        lane = lax.broadcasted_iota(jnp.int32, (512, 128), 1)
        half = (lane % 64).astype(jnp.float32)
        freq = jnp.exp(half * (-2.0 * math.log(THETA) / 128))
        ang = pos.astype(jnp.float32) * freq
        cos_t[...] = jnp.cos(ang)
        s = jnp.sin(ang)
        sin_t[...] = jnp.where(lane < 64, -s, s)

    outs = []

    def put(src, dst, n):
        cp = pltpu.make_async_copy(src, dst, out_sem.at[n])
        cp.start()
        outs.append(cp)

    def put_kv(half):
        put(kvb.at[half], kv_out.at[half], half)

    def put_state(hp):
        put(st_m.at[hp], m_out.at[hp], 3 + hp)
        put(st_l.at[hp], l_out.at[hp], 7 + hp)
        put(st_o.at[hp], o_out.at[hp], 11 + hp)

    def attend(hp):
        q = qs[1, pl.ds(hp * 512, 512), :]
        carry = (
            jnp.full((512, 1), NEG, jnp.float32),
            jnp.zeros((512, 128), jnp.float32),
            jnp.zeros((512, 128), jnp.float32),
        )
        m, l, o = lax.fori_loop(0, 4, lambda t, st: absorb(q, kvb, 0, t, st, None), carry)
        st_m[hp] = jnp.broadcast_to(m, (512, 128))
        st_l[hp] = l
        st_o[hp] = o

    local[0].wait()
    local[1].wait()
    own(0)
    local[2].wait()
    xown(0)
    for cp in local[3:]:
        cp.wait()
    tables()
    own(1)
    xown(1)
    relay_own(0)
    xrelay(0, 0)
    xpartner(0)
    partner(0)
    own(2)
    xown(2)
    xrelay(0, 1)
    xrelay(1, 0)
    xpartner(1)
    relay_partner(0)
    relay_own(1)
    partner(1)
    last(0)
    xlast(0)
    own(3)
    xown(3)
    xrelay(1, 1)
    xrelay(2, 0)
    xpartner(2)
    relay_partner(1)
    relay_own(2)
    partner(2)
    other_core(0)
    xlast(1)
    make_kv(0)
    last(1)
    own(S_E)
    xrelay(2, 1)
    xrelay(3, 0)
    xpartner(3)
    relay_partner(2)
    relay_own(3)
    relay_own(S_E)
    partner(S_E)
    partner(3)
    own(4)
    other_core(1)
    make_q(0, 0)
    xrelay(3, 1)
    last(2)
    xlast(2)
    relay_partner(S_E)
    relay_partner(3)
    other_core(2)
    make_q(1, 0)
    relay_own(4)
    partner(4)
    last(S_E)
    other_core(S_E)
    put_kv(0)
    xlast(3)
    make_kv(1)
    last(3)
    make_q(0, 1)
    own(S_L)
    relay_partner(4)
    make_q(1, 1)
    other_core(3)
    make_q(2, 0)
    relay_own(S_L)
    partner(S_L)
    make_q(2, 1)
    attend(0)
    relay_partner(S_L)
    last(4)
    attend(1)
    last(S_L)
    put_state(0)
    attend(2)
    other_core(4)
    make_q(3, 0)
    make_q(3, 1)
    other_core(S_L)
    put_kv(1)
    put_state(1)
    attend(3)
    put_state(2)
    put_state(3)
    put(qs, q_out, 2)
    for cp in sends:
        cp.wait_send()
    for cp in outs:
        cp.wait()


def absorb(q, kv, seg, t, state, vis):
    m, l, o = state
    kt = kv[seg, pl.ds(t * 4, 4), :, 0:128].reshape(KT, 128)
    vt = kv[seg, pl.ds(t * 4, 4), :, 128:256].reshape(KT, 128)
    s = lax.dot_general(q, kt, (((1,), (1,)), ((), ())), preferred_element_type=jnp.float32)
    if vis is not None:
        s = jnp.where(vis, s, NEG)
    mx = s[:, 0:128]
    for u in range(1, KT // 128):
        mx = jnp.maximum(mx, s[:, u * 128:(u + 1) * 128])
    mnew = jnp.maximum(m, jnp.max(mx, axis=1, keepdims=True) * EXP2_SCALE)
    pr = jnp.exp2(s * EXP2_SCALE - mnew)
    a = jnp.exp2(m - mnew)
    ps = pr[:, 0:128]
    for u in range(1, KT // 128):
        ps = ps + pr[:, u * 128:(u + 1) * 128]
    l = l * a + ps
    o = o * a + jnp.dot(pr.astype(jnp.bfloat16), vt, preferred_element_type=jnp.float32)
    return mnew, l, o


def gather_project(pair_ids, tokens, wq, wk, wv, bq, bk, bv):
    vmem = pl.BlockSpec(memory_space=pltpu.VMEM)
    hbm = pl.BlockSpec(memory_space=pl.ANY)
    state = jax.ShapeDtypeStruct((4, 512, 128), jnp.float32)
    return pl.pallas_call(
        kernel,
        out_shape=(
            jax.ShapeDtypeStruct((2, 2048, 128), jnp.bfloat16),
            jax.ShapeDtypeStruct((2, 16, 256, 256), jnp.bfloat16),
            state, state, state,
        ),
        in_specs=[pl.BlockSpec(memory_space=pltpu.SMEM), hbm, hbm, hbm, hbm, vmem, vmem, vmem],
        out_specs=(hbm,) * 5,
        scratch_shapes=[
            pltpu.VMEM((XS, 8, 128, 1024), jnp.bfloat16),
            pltpu.VMEM((5, 16, 512, 256), jnp.bfloat16),
            pltpu.VMEM((2, 16, 256, 256), jnp.bfloat16),
            pltpu.VMEM((2, 2048, 128), jnp.bfloat16),
            pltpu.VMEM((256, 256), jnp.float32),
            pltpu.VMEM((512, 128), jnp.float32),
            pltpu.VMEM((512, 128), jnp.float32),
            pltpu.VMEM((4, 512, 128), jnp.float32),
            pltpu.VMEM((4, 512, 128), jnp.float32),
            pltpu.VMEM((4, 512, 128), jnp.float32),
            pltpu.SemaphoreType.DMA((10,)),
            pltpu.SemaphoreType.DMA((15,)),
            pltpu.SemaphoreType.DMA((SLOTS, 19)),
            pltpu.SemaphoreType.DMA((SLOTS, 19)),
            pltpu.SemaphoreType.DMA((XS, 9)),
            pltpu.SemaphoreType.DMA((XS, 9)),
        ],
        compiler_params=pltpu.CompilerParams(
            collective_id=0, has_side_effects=True, vmem_limit_bytes=63 * 2**20
        ),
    )(pair_ids, tokens, wq, wk, wv, bq, bk, bv)


def attn_kernel(pair_ref, q_hbm, kv_hbm, m_hbm, l_hbm, o_hbm, out_ref, q, kv, m0, l0, o0, sem, *, G):
    def cp(half, j):
        slot = pair_ref[j] if half == 0 else 15 - pair_ref[j]
        return pltpu.make_async_copy(kv_hbm.at[half, j], kv.at[half, slot], sem.at[half, j])

    rest = [
        pltpu.make_async_copy(a, b, sem.at[2, n])
        for n, (a, b) in enumerate(
            ((q_hbm.at[0], q.at[0]), (q_hbm.at[1], q.at[1]), (m_hbm, m0), (l_hbm, l0), (o_hbm, o0))
        )
    ]
    rest[0].start()
    for half in range(2):

        @pl.loop(0, 16)
        def _(j):
            cp(half, j).start()

        for r in rest[1:] if half else ():
            r.start()
    p = pair_ref[lax.axis_index("gy")]
    R = G * 256
    for half in range(2):

        @pl.loop(0, 16)
        def _(j):
            cp(half, j).wait()

        for r in rest[1:] if half else rest[:1]:
            r.wait()
        blk = p if half == 0 else 15 - p
        full = blk // 4

        @pl.loop(0, 8 // G)
        def _(i):
            rows = pl.ds(pl.multiple_of(i * R, R), R)
            qt = q[half, rows, :]
            if half:
                parts = [
                    jnp.concatenate([r[i * (G // 2) + g] for g in range(G // 2)], axis=0)
                    for r in (m0, l0, o0)
                ]
                state = (parts[0][:, 0:1], parts[1], parts[2])
            else:
                state = (
                    jnp.full((R, 1), NEG, jnp.float32),
                    jnp.zeros((R, 128), jnp.float32),
                    jnp.zeros((R, 128), jnp.float32),
                )
            ahead = lax.broadcasted_iota(jnp.int32, (R, KT), 1) - (
                lax.broadcasted_iota(jnp.int32, (R, KT), 0) % 256
            )
            state = absorb(qt, kv, half, full, state, ahead <= (blk - full * 4) * 256)
            m, l, o = lax.fori_loop(
                0, full, lambda t, st: absorb(qt, kv, half, t, st, None), state
            )
            o = (o / jnp.sum(l, axis=1, keepdims=True)).astype(jnp.bfloat16)
            for g in range(G):
                out_ref[half * 256:(half + 1) * 256, pl.ds(pl.multiple_of((i * G + g) * 128, 128), 128)] = (
                    o[g * 256:(g + 1) * 256]
                )


def on_device(tokens, pair_ids, wq, wk, wv, bq, bk, bv):
    q, kv, m, l, o = gather_project(pair_ids, tokens, wq, wk, wv, bq, bk, bv)
    hbm = pl.BlockSpec(memory_space=pl.ANY)
    return pl.pallas_call(
        functools.partial(attn_kernel, G=4),
        out_shape=jax.ShapeDtypeStruct((512, 1024), jnp.bfloat16),
        in_specs=[pl.BlockSpec(memory_space=pltpu.SMEM)] + [hbm] * 5,
        out_specs=pl.BlockSpec(memory_space=pltpu.VMEM),
        scratch_shapes=[
            pltpu.VMEM((2, 2048, 128), jnp.bfloat16),
            pltpu.VMEM((2, 16, 256, 256), jnp.bfloat16),
            pltpu.VMEM((4, 512, 128), jnp.float32),
            pltpu.VMEM((4, 512, 128), jnp.float32),
            pltpu.VMEM((4, 512, 128), jnp.float32),
            pltpu.SemaphoreType.DMA((3, 16)),
        ],
        compiler_params=pltpu.CompilerParams(vmem_limit_bytes=60 * 2**20),
    )(pair_ids, q, kv, m, l, o)


def solution(mesh):
    placed = (P("gy", "gx"), P(), P("gy", "gx"), P("gy", "gx"), P("gy", "gx"), P("gx"), P("gx"), P("gx"))
    return jax.shard_map(
        on_device, mesh=mesh, in_specs=placed, out_specs=P("gy", "gx"), check_vma=False
    )
```

```python
import functools
import math

import jax
import jax.numpy as jnp
from jax import lax
from jax.experimental import pallas as pl
from jax.experimental.pallas import tpu as pltpu
from jax.sharding import PartitionSpec as P

THETA = 1000000.0
EXP2_SCALE = math.log2(math.e) / math.sqrt(128)
NEG = -1e30
MESH = pl.DeviceIdType.MESH

XS = 4
SLOTS = 7
S_E, S_L = 5, 6
KT = 1024
VIA_Z = (4, 16)


def kernel(
    pair_ref, x_hbm, wq_hbm, wk_hbm, wv_hbm, bq_ref, bk_ref, bv_ref,
    q_out, kv_out, m_out, l_out, o_out,
    xb, wb, kvb, qs, acc, cos_t, sin_t, st_m, st_l, st_o, loc_sem, out_sem, ws, wr, xs, xr,
):
    gx, gy = lax.axis_index("gx"), lax.axis_index("gy")
    y, zl = gx // 2, gx % 2
    zh, x, c = gy // 8, (gy // 2) % 4, gy % 2

    def at(dx=0, dy=0, dzh=0, dzl=0, dc=0):
        return (
            ((y + dy) % 4) * 2 + (zl + dzl) % 2,
            (((zh + dzh) % 2) * 4 + (x + dx) % 4) * 2 + (c + dc) % 2,
        )

    core, xp, xm, yp, ym, zfar, znear = (
        at(dc=1), at(dx=1), at(dx=3), at(dy=1), at(dy=3), at(dzh=1), at(dzl=1)
    )

    def block(plane, dx, dc=0):
        return (((zh + plane) % 2) * 4 + (x + dx) % 4) * 2 + (c + dc) % 2

    def xblock(plane, dy):
        return ((y + dy) % 4) * 2 + (zl + plane) % 2

    local = []

    def load(src, dst, n):
        cp = pltpu.make_async_copy(src, dst, loc_sem.at[n])
        cp.start()
        local.append(cp)

    load(wk_hbm, wb.at[0, gy, :, pl.ds(0, 128)], 0)
    load(wv_hbm, wb.at[0, gy, :, pl.ds(128, 128)], 1)
    for r in range(XS):
        load(x_hbm.at[pl.ds(r * 128, 128)], xb.at[r, gx], 2 + r)
    for t in range(1, 5):
        load(wq_hbm.at[:, pl.ds((t - 1) * 256, 256)], wb.at[t, gy], 5 + t)

    barrier = pltpu.get_barrier_semaphore()
    for n in (core, xp, xm, yp, ym, zfar, znear):
        pl.semaphore_signal(barrier, inc=1, device_id=n, device_id_type=MESH)
    pl.semaphore_wait(barrier, 7)

    sends = []

    def send(src, dst, ssem, rsem, dev):
        cp = pltpu.make_async_remote_copy(
            src_ref=src, dst_ref=dst, send_sem=ssem, recv_sem=rsem, device_id=dev,
            device_id_type=MESH,
        )
        cp.start()
        sends.append(cp)

    def arrived(ref, sem):
        pltpu.make_async_copy(ref, ref, sem).wait()

    def blk(s, j):
        return wb.at[s, j] if s < S_E else kvb.at[s - S_E, j]

    def cuts(s):
        n = 512 if s < S_E else 256
        v = n * VIA_Z[0] // VIA_Z[1]
        return pl.ds(0, n // 2), pl.ds(n // 2, n // 2), pl.ds(0, n - v), pl.ds(n - v, v)

    P0, OM, OP, PM, PP, PMV, PPV, O2A, O2B, P2A, P2B, D = range(12)
    doff = {(0, 0): 0, (0, 3): 1, (0, 1): 2, (1, 0): 3, (1, 3): 4, (1, 1): 5, (0, 2): 6, (1, 2): 7}

    def wsend(s, ref, role, dev):
        send(ref, ref, ws.at[s, role], wr.at[s, role], dev)

    def d2d(s, plane, dx):
        wsend(s, blk(s, block(plane, dx)), D + doff[(plane, dx)], core)

    def own(s):
        b = blk(s, gy)
        wsend(s, b, P0, zfar)
        wsend(s, b, OM, xp)
        wsend(s, b, OP, xm)
        d2d(s, 0, 0)

    def relay_own(s):
        lo, hi, u, v = cuts(s)
        b = blk(s, block(0, 3))
        arrived(b, wr.at[s, OM])
        wsend(s, b.at[lo], O2A, xp)
        wsend(s, b.at[v], PMV, zfar)
        d2d(s, 0, 3)
        b = blk(s, block(0, 1))
        arrived(b, wr.at[s, OP])
        wsend(s, b.at[hi], O2B, xm)
        wsend(s, b.at[v], PPV, zfar)
        d2d(s, 0, 1)

    def partner(s):
        lo, hi, u, v = cuts(s)
        b = blk(s, block(1, 0))
        arrived(b, wr.at[s, P0])
        wsend(s, b.at[u], PM, xp)
        wsend(s, b.at[u], PP, xm)
        d2d(s, 1, 0)

    def relay_partner(s):
        lo, hi, u, v = cuts(s)
        b = blk(s, block(1, 3))
        arrived(b.at[u], wr.at[s, PM])
        arrived(b.at[v], wr.at[s, PMV])
        wsend(s, b.at[lo], P2A, xp)
        d2d(s, 1, 3)
        b = blk(s, block(1, 1))
        arrived(b.at[u], wr.at[s, PP])
        arrived(b.at[v], wr.at[s, PPV])
        wsend(s, b.at[hi], P2B, xm)
        d2d(s, 1, 1)

    def last(s):
        lo, hi, u, v = cuts(s)
        for plane, ra, rb in ((0, O2A, O2B), (1, P2A, P2B)):
            b = blk(s, block(plane, 2))
            arrived(b.at[lo], wr.at[s, ra])
            arrived(b.at[hi], wr.at[s, rb])
            d2d(s, plane, 2)

    def other_core(s):
        for (plane, dx), d in doff.items():
            arrived(blk(s, block(plane, dx, 1)), wr.at[s, D + d])

    XZ, XOM, XOP, XPM, XPP, XO2A, XO2B, XP2A, XP2B = range(9)
    xlo, xhi = pl.ds(0, 64), pl.ds(64, 64)

    def xsend(t, ref, role, dev):
        send(ref, ref, xs.at[t, role], xr.at[t, role], dev)

    def xown(t):
        b = xb.at[t, gx]
        xsend(t, b, XZ, znear)
        xsend(t, b, XOM, yp)
        xsend(t, b, XOP, ym)

    def xrelay(t, plane):
        rm, rp, ra, rb = (XOM, XOP, XO2A, XO2B) if plane == 0 else (XPM, XPP, XP2A, XP2B)
        b = xb.at[t, xblock(plane, 3)]
        arrived(b, xr.at[t, rm])
        xsend(t, b.at[xlo], ra, yp)
        b = xb.at[t, xblock(plane, 1)]
        arrived(b, xr.at[t, rp])
        xsend(t, b.at[xhi], rb, ym)

    def xpartner(t):
        b = xb.at[t, xblock(1, 0)]
        arrived(b, xr.at[t, XZ])
        xsend(t, b, XPM, yp)
        xsend(t, b, XPP, ym)

    def xlast(t):
        for plane, ra, rb in ((0, XO2A, XO2B), (1, XP2A, XP2B)):
            b = xb.at[t, xblock(plane, 2)]
            arrived(b.at[xlo], xr.at[t, ra])
            arrived(b.at[xhi], xr.at[t, rb])

    def project(s, half):
        total = None
        for b in range(8):
            part = jnp.dot(
                xb[pl.ds(2 * half, 2), b].reshape(256, 1024),
                wb[s, pl.ds(2 * b, 2)].reshape(1024, 256),
                preferred_element_type=jnp.float32,
            )
            total = part if total is None else total + part
        acc[...] = total

    def rope(u, half):
        r = pl.ds(half * 256, 256)
        return u * cos_t[r, :] + pltpu.roll(u, 64, 1) * sin_t[r, :]

    def make_kv(half):
        project(0, half)
        kvb[half, gy, :, 0:128] = rope(
            acc[:, 0:128] + bk_ref[...].astype(jnp.float32).reshape(1, 128), half
        ).astype(jnp.bfloat16)
        kvb[half, gy, :, 128:256] = (
            acc[:, 128:256] + bv_ref[...].astype(jnp.float32).reshape(1, 128)
        ).astype(jnp.bfloat16)

    def make_q(hp, half):
        project(hp + 1, half)
        for g in range(2):
            h = 2 * hp + g
            u = acc[:, g * 128:(g + 1) * 128] + bq_ref[h * 128:(h + 1) * 128].astype(jnp.float32).reshape(1, 128)
            qs[half, pl.ds(h * 256, 256), :] = rope(u, half).astype(jnp.bfloat16)

    def tables():
        p = pair_ref[gy]
        row = lax.broadcasted_iota(jnp.int32, (512, 128), 0)
        pos = jnp.where(row < 256, p * 256 + row, (31 - p) * 256 + row - 256)
        lane = lax.broadcasted_iota(jnp.int32, (512, 128), 1)
        half = (lane % 64).astype(jnp.float32)
        freq = jnp.exp(half * (-2.0 * math.log(THETA) / 128))
        ang = pos.astype(jnp.float32) * freq
        cos_t[...] = jnp.cos(ang)
        s = jnp.sin(ang)
        sin_t[...] = jnp.where(lane < 64, -s, s)

    outs = []

    def put(src, dst, n):
        cp = pltpu.make_async_copy(src, dst, out_sem.at[n])
        cp.start()
        outs.append(cp)

    def put_kv(half):
        put(kvb.at[half], kv_out.at[half], half)

    def put_state(hp):
        put(st_m.at[hp], m_out.at[hp], 3 + hp)
        put(st_l.at[hp], l_out.at[hp], 7 + hp)
        put(st_o.at[hp], o_out.at[hp], 11 + hp)

    def attend(hp):
        q = qs[1, pl.ds(hp * 512, 512), :]
        carry = (
            jnp.full((512, 1), NEG, jnp.float32),
            jnp.zeros((512, 128), jnp.float32),
            jnp.zeros((512, 128), jnp.float32),
        )
        m, l, o = lax.fori_loop(0, 4, lambda t, st: absorb(q, kvb, 0, t, st, None), carry)
        st_m[hp] = jnp.broadcast_to(m, (512, 128))
        st_l[hp] = l
        st_o[hp] = o

    local[0].wait()
    local[1].wait()
    own(0)
    local[2].wait()
    xown(0)
    for cp in local[3:]:
        cp.wait()
    tables()
    own(1)
    xown(1)
    relay_own(0)
    xrelay(0, 0)
    xpartner(0)
    partner(0)
    own(2)
    xown(2)
    xrelay(0, 1)
    xrelay(1, 0)
    xpartner(1)
    relay_partner(0)
    relay_own(1)
    partner(1)
    last(0)
    xlast(0)
    own(3)
    xown(3)
    xrelay(1, 1)
    xrelay(2, 0)
    xpartner(2)
    relay_partner(1)
    relay_own(2)
    partner(2)
    other_core(0)
    xlast(1)
    make_kv(0)
    last(1)
    own(S_E)
    xrelay(2, 1)
    xrelay(3, 0)
    xpartner(3)
    relay_partner(2)
    relay_own(3)
    relay_own(S_E)
    partner(S_E)
    partner(3)
    own(4)
    other_core(1)
    make_q(0, 0)
    xrelay(3, 1)
    last(2)
    xlast(2)
    relay_partner(S_E)
    relay_partner(3)
    other_core(2)
    make_q(1, 0)
    relay_own(4)
    partner(4)
    last(S_E)
    other_core(S_E)
    put_kv(0)
    xlast(3)
    make_kv(1)
    last(3)
    make_q(0, 1)
    own(S_L)
    relay_partner(4)
    make_q(1, 1)
    other_core(3)
    make_q(2, 0)
    relay_own(S_L)
    partner(S_L)
    make_q(2, 1)
    attend(0)
    relay_partner(S_L)
    last(4)
    attend(1)
    last(S_L)
    put_state(0)
    attend(2)
    other_core(4)
    make_q(3, 0)
    make_q(3, 1)
    put_state(1)
    attend(3)
    other_core(S_L)
    put_kv(1)
    put_state(2)
    put_state(3)
    put(qs, q_out, 2)
    for cp in sends:
        cp.wait_send()
    for cp in outs:
        cp.wait()


def absorb(q, kv, seg, t, state, vis):
    m, l, o = state
    kt = kv[seg, pl.ds(t * 4, 4), :, 0:128].reshape(KT, 128)
    vt = kv[seg, pl.ds(t * 4, 4), :, 128:256].reshape(KT, 128)
    s = lax.dot_general(q, kt, (((1,), (1,)), ((), ())), preferred_element_type=jnp.float32)
    if vis is not None:
        s = jnp.where(vis, s, NEG)
    mx = s[:, 0:128]
    for u in range(1, KT // 128):
        mx = jnp.maximum(mx, s[:, u * 128:(u + 1) * 128])
    mnew = jnp.maximum(m, jnp.max(mx, axis=1, keepdims=True) * EXP2_SCALE)
    pr = jnp.exp2(s * EXP2_SCALE - mnew)
    a = jnp.exp2(m - mnew)
    ps = pr[:, 0:128]
    for u in range(1, KT // 128):
        ps = ps + pr[:, u * 128:(u + 1) * 128]
    l = l * a + ps
    o = o * a + jnp.dot(pr.astype(jnp.bfloat16), vt, preferred_element_type=jnp.float32)
    return mnew, l, o


def gather_project(pair_ids, tokens, wq, wk, wv, bq, bk, bv):
    vmem = pl.BlockSpec(memory_space=pltpu.VMEM)
    hbm = pl.BlockSpec(memory_space=pl.ANY)
    state = jax.ShapeDtypeStruct((4, 512, 128), jnp.float32)
    return pl.pallas_call(
        kernel,
        out_shape=(
            jax.ShapeDtypeStruct((2, 2048, 128), jnp.bfloat16),
            jax.ShapeDtypeStruct((2, 16, 256, 256), jnp.bfloat16),
            state, state, state,
        ),
        in_specs=[pl.BlockSpec(memory_space=pltpu.SMEM), hbm, hbm, hbm, hbm, vmem, vmem, vmem],
        out_specs=(hbm,) * 5,
        scratch_shapes=[
            pltpu.VMEM((XS, 8, 128, 1024), jnp.bfloat16),
            pltpu.VMEM((5, 16, 512, 256), jnp.bfloat16),
            pltpu.VMEM((2, 16, 256, 256), jnp.bfloat16),
            pltpu.VMEM((2, 2048, 128), jnp.bfloat16),
            pltpu.VMEM((256, 256), jnp.float32),
            pltpu.VMEM((512, 128), jnp.float32),
            pltpu.VMEM((512, 128), jnp.float32),
            pltpu.VMEM((4, 512, 128), jnp.float32),
            pltpu.VMEM((4, 512, 128), jnp.float32),
            pltpu.VMEM((4, 512, 128), jnp.float32),
            pltpu.SemaphoreType.DMA((10,)),
            pltpu.SemaphoreType.DMA((15,)),
            pltpu.SemaphoreType.DMA((SLOTS, 19)),
            pltpu.SemaphoreType.DMA((SLOTS, 19)),
            pltpu.SemaphoreType.DMA((XS, 9)),
            pltpu.SemaphoreType.DMA((XS, 9)),
        ],
        compiler_params=pltpu.CompilerParams(
            collective_id=0, has_side_effects=True, vmem_limit_bytes=63 * 2**20
        ),
    )(pair_ids, tokens, wq, wk, wv, bq, bk, bv)


def attn_kernel(pair_ref, q_hbm, kv_hbm, m_hbm, l_hbm, o_hbm, out_ref, q, kv, m0, l0, o0, sem, *, G):
    def cp(half, j):
        slot = pair_ref[j] if half == 0 else 15 - pair_ref[j]
        return pltpu.make_async_copy(kv_hbm.at[half, j], kv.at[half, slot], sem.at[half, j])

    rest = [
        pltpu.make_async_copy(a, b, sem.at[2, n])
        for n, (a, b) in enumerate(
            ((q_hbm.at[0], q.at[0]), (q_hbm.at[1], q.at[1]), (m_hbm, m0), (l_hbm, l0), (o_hbm, o0))
        )
    ]
    rest[0].start()
    for half in range(2):

        @pl.loop(0, 16)
        def _(j):
            cp(half, j).start()

        for r in rest[1:] if half else ():
            r.start()
    p = pair_ref[lax.axis_index("gy")]
    R = G * 256
    for half in range(2):

        @pl.loop(0, 16)
        def _(j):
            cp(half, j).wait()

        for r in rest[1:] if half else rest[:1]:
            r.wait()
        blk = p if half == 0 else 15 - p
        full = blk // 4

        @pl.loop(0, 8 // G)
        def _(i):
            rows = pl.ds(pl.multiple_of(i * R, R), R)
            qt = q[half, rows, :]
            if half:
                parts = [
                    jnp.concatenate([r[i * (G // 2) + g] for g in range(G // 2)], axis=0)
                    for r in (m0, l0, o0)
                ]
                state = (parts[0][:, 0:1], parts[1], parts[2])
            else:
                state = (
                    jnp.full((R, 1), NEG, jnp.float32),
                    jnp.zeros((R, 128), jnp.float32),
                    jnp.zeros((R, 128), jnp.float32),
                )
            ahead = lax.broadcasted_iota(jnp.int32, (R, KT), 1) - (
                lax.broadcasted_iota(jnp.int32, (R, KT), 0) % 256
            )
            state = absorb(qt, kv, half, full, state, ahead <= (blk - full * 4) * 256)
            m, l, o = lax.fori_loop(
                0, full, lambda t, st: absorb(qt, kv, half, t, st, None), state
            )
            o = (o / jnp.sum(l, axis=1, keepdims=True)).astype(jnp.bfloat16)
            for g in range(G):
                out_ref[half * 256:(half + 1) * 256, pl.ds(pl.multiple_of((i * G + g) * 128, 128), 128)] = (
                    o[g * 256:(g + 1) * 256]
                )


def on_device(tokens, pair_ids, wq, wk, wv, bq, bk, bv):
    q, kv, m, l, o = gather_project(pair_ids, tokens, wq, wk, wv, bq, bk, bv)
    hbm = pl.BlockSpec(memory_space=pl.ANY)
    return pl.pallas_call(
        functools.partial(attn_kernel, G=4),
        out_shape=jax.ShapeDtypeStruct((512, 1024), jnp.bfloat16),
        in_specs=[pl.BlockSpec(memory_space=pltpu.SMEM)] + [hbm] * 5,
        out_specs=pl.BlockSpec(memory_space=pltpu.VMEM),
        scratch_shapes=[
            pltpu.VMEM((2, 2048, 128), jnp.bfloat16),
            pltpu.VMEM((2, 16, 256, 256), jnp.bfloat16),
            pltpu.VMEM((4, 512, 128), jnp.float32),
            pltpu.VMEM((4, 512, 128), jnp.float32),
            pltpu.VMEM((4, 512, 128), jnp.float32),
            pltpu.SemaphoreType.DMA((3, 16)),
        ],
        compiler_params=pltpu.CompilerParams(vmem_limit_bytes=60 * 2**20),
    )(pair_ids, q, kv, m, l, o)


def solution(mesh):
    placed = (P("gy", "gx"), P(), P("gy", "gx"), P("gy", "gx"), P("gy", "gx"), P("gx"), P("gx"), P("gx"))
    return jax.shard_map(
        on_device, mesh=mesh, in_specs=placed, out_specs=P("gy", "gx"), check_vma=False
    )
```
